32 devices in a mesh: row: 4 (over x, core), col: 4 (over z), layer: 2 (over y).
Axes of the slice: x: 2, y: 2, z: 4, core: 2. Of those that a mesh axis runs over, the one named last changes fastest.
Arguments:
- left_factor: float32 [6144, 8192], P('row', 'col'), may hold values from -6 to 6
- right_factor: float32 [8192, 6144], P('row', 'col'), may hold values from -0.0625 to 0.0625
Outputs:
- product: float32 [6144, 6144], P(('row', 'layer'), 'col')
The draws below stay inside these ranges and needn't reach their ends.
All inputs are finite; a program needn't handle non-finite values.
Results may differ from the reference program's by a relative error of at most 0.000073.
Values sent between devices are 32-bit elements; how exact they have to be, the bound alone decides.
A program may use at most 192 MiB of HBM per device.

```python
import jax
import jax.numpy as jnp
from jax import lax

K = 8192
M = 6144
NC = 6144


def spiked(drawn, stream_key, source, target, blocks, factor):
    def block_of(dim):
        return (jnp.arange(drawn.shape[dim]) // (drawn.shape[dim] // blocks)).reshape((-1,) + (1,) * (drawn.ndim - 1 - dim))

    one_side = jax.random.permutation(stream_key, blocks)[block_of(target)]
    second = (block_of(target) + blocks // 2) % blocks
    return jnp.where((block_of(source) == one_side) | (block_of(source) == second), factor * drawn, drawn)


def block_scale(rng, dims, split, least, top_value):
    gain = 1.0
    for position, shards_of in split:
        draws = jax.random.uniform(jax.random.fold_in(jax.random.fold_in(rng, 6), position), (shards_of,), jnp.float32, least / len(split), top_value / len(split))
        gain = gain * jnp.repeat(jnp.exp(draws), dims[position] // shards_of).reshape((-1,) + (1,) * (len(dims) - 1 - position))
    return gain


def gaussian(key, dims, scale, reach, pieces=(), held_as=jnp.bfloat16):
    drawn = scale * jax.random.normal(key, dims, jnp.float32)
    if pieces:
        drawn = drawn * block_scale(key, dims, pieces, -0.22, 0.18)
    return jnp.clip(drawn, -reach, reach).astype(held_as)


def noise_with(key, dims, spread, most, cuts, heavy, dtype=jnp.bfloat16):
    drawn = spread * jax.random.normal(key, dims, jnp.float32)
    if cuts:
        drawn = drawn * block_scale(key, dims, cuts, -0.22, 0.18)
    return jnp.clip(spiked(drawn, jax.random.fold_in(key, 3), *heavy), -most, most).astype(dtype)


def setup_inputs(seed: int = 0) -> dict:
    seeds = jax.random.split(jax.random.key(seed), 3)
    return {
        "left_factor": noise_with(seeds[0], (M, K), 1.0, 6.0, ((0, 4), (1, 4)), (1, 0, 4, 2.0), jnp.float32),
        "right_factor": gaussian(seeds[1], (K, NC), K ** -0.5, 0.0625, ((0, 4), (1, 4)), jnp.float32),
    }


def reference(left_factor, right_factor):
    return jnp.dot(left_factor, right_factor, precision=lax.Precision.HIGHEST, preferred_element_type=jnp.float32)
```

```python
import jax
import jax.numpy as jnp
from jax import lax
from jax.experimental import pallas as pl
from jax.experimental.pallas import tpu as pltpu
from jax.sharding import PartitionSpec as P

MESH = pl.DeviceIdType.MESH
PARTS = (4, 4, 4, 2, 2)
LANES = 512
PIECES = 4
SUBS = 2


def product(left, right):
    return jnp.dot(
        left,
        right,
        precision=lax.Precision.HIGH,
        preferred_element_type=jnp.float32,
    )


def gathered(left_factor, right_factor):
    layers = lax.axis_size("layer")
    rows = left_factor.shape[0] // layers
    left = lax.dynamic_slice_in_dim(left_factor, lax.axis_index("layer") * rows, rows, 0)
    left = lax.all_gather(left, "col", axis=1, tiled=True)
    right = lax.all_gather(right_factor, "row", axis=0, tiled=True)
    return product(left, right)


def keys():
    n, table = 0, {}
    counts = dict(AE=len(PARTS), AB=len(PARTS), AO=len(PARTS), AF=len(PARTS), CX=len(PARTS))
    counts.update(X=SUBS, XE=SUBS, MC=2, MX=PIECES, MY=PIECES, MF=2 * PIECES)
    counts.update(P1=SUBS, P2O=SUBS, P2F=SUBS, C0=SUBS, C1=SUBS, C2=SUBS, C3=SUBS)
    for name, count in counts.items():
        for i in range(count):
            table[name, i] = n
            n += 1
    return table


KEYS = keys()


def kernel(left, right, out, abuf, bmain, bx, acc, cx, stage, atile, btile, send, recv, asem, bsem, osem):
    row, z, layer = (lax.axis_index(name) for name in ("row", "col", "layer"))
    rows, wide = acc.shape
    depth = right.shape[0]
    half = depth // 2
    unit = rows // sum(PARTS)
    sizes = [part * unit for part in PARTS]
    starts = [sum(sizes[:i]) for i in range(len(sizes))]
    core = lax.rem(row, 2)
    low = z < 2
    edge = (z == 0) | (z == 3)
    near = (row // 2) == (z // 2)
    farther = jnp.where(near, 0, 1)
    row_x = lax.rem(row + 2, 4)
    row_c = row + 1 - 2 * core
    outer = jnp.where(low, z - 1, z + 1)
    inner = jnp.where(low, z + 1, z - 1)
    flip = 1 - layer
    by_x, by_c, by_y = {"row": row_x}, {"row": row_c}, {"layer": flip}
    by_out, by_in = {"col": outer}, {"col": inner}
    first_x = core == 0
    by_1 = {"row": jnp.where(first_x, row_x, row), "layer": jnp.where(first_x, layer, flip)}
    by_2 = {"row": jnp.where(first_x, row, row_x), "layer": jnp.where(first_x, flip, layer)}
    my_rows = layer * rows

    def remote(src, dst, key, device):
        k = KEYS[key]
        return pltpu.make_async_remote_copy(
            src_ref=src, dst_ref=dst, send_sem=send.at[k], recv_sem=recv.at[k], device_id=device, device_id_type=MESH
        )

    sent = []

    def put(src, dst, key, device):
        copy = remote(src, dst, key, device)
        copy.start()
        sent.append(copy)

    def got(dst, key):
        remote(dst, dst, key, by_c).wait_recv()

    def own_a(i):
        return left.at[pl.ds(my_rows + starts[i], sizes[i]), :]

    def slot_a(slot, i):
        return abuf.at[slot, pl.ds(starts[i], sizes[i]), :]

    def aligned(value):
        return pl.multiple_of(value, 128)

    cut = half // PIECES
    sub = half // 2 // SUBS

    def main(slot, which, p):
        return bmain.at[slot, pl.ds(aligned(which * half + p * cut), cut), :]

    def mine(p):
        return right.at[pl.ds(aligned(layer * half + p * cut), cut), :]

    def extra(q, far, which, t):
        return bx.at[q, pl.ds(aligned(which * half + far * (half // 2) + t * sub), sub), :]

    def extra_source(ref, far, t):
        return ref.at[pl.ds(aligned(layer * half + far * (half // 2) + t * sub), sub), :]

    spot = jnp.where(near, 1, 0)
    pair_1 = (jnp.where(first_x, 1 - spot, spot), jnp.where(first_x, layer, flip))
    pair_2 = (jnp.where(first_x, spot, 1 - spot), jnp.where(first_x, flip, layer))
    pair_3 = (1 - spot, flip)
    twin_1 = (jnp.where(first_x, spot, 1 - spot), jnp.where(first_x, flip, layer))
    twin_2 = (jnp.where(first_x, 1 - spot, spot), jnp.where(first_x, layer, flip))

    def load_a(slot, size, own, block, start, col):
        where = pl.ds(aligned(col), half)

        @pl.when(own)
        def _():
            pltpu.make_async_copy(
                left.at[pl.ds(my_rows + start, size), where], atile.at[slot, pl.ds(0, size), :], asem.at[slot]
            ).start()

        @pl.when(jnp.logical_not(own))
        def _():
            pltpu.make_async_copy(
                abuf.at[block, pl.ds(start, size), where], atile.at[slot, pl.ds(0, size), :], asem.at[slot]
            ).start()

    def wait_a(slot, size):
        view = atile.at[slot, pl.ds(0, size), :]
        pltpu.make_async_copy(view, view, asem.at[slot]).wait()

    def load_b(slot, term, which):
        where = pl.ds(aligned(which * half), half)

        @pl.when(term == 0)
        def _():
            pltpu.make_async_copy(right.at[where, :], btile.at[slot], bsem.at[slot]).start()

        @pl.when(term > 0)
        def _():
            pltpu.make_async_copy(bmain.at[jnp.maximum(term - 1, 0), where, :], btile.at[slot], bsem.at[slot]).start()

    def wait_b(slot):
        pltpu.make_async_copy(btile.at[slot], btile.at[slot], bsem.at[slot]).wait()

    def owner(term):
        return jnp.where(term == 0, row, jnp.where(term == 1, row_c, jnp.where(term == 2, row_x, 3 - row)))

    def place(block):
        turned = jnp.where(low, block, 3 - block)
        return jnp.maximum(turned - 1, 0)

    def multiply(total, start, size, slot, weights):
        def lanes(t, carry):
            columns = pl.ds(pl.multiple_of(t * LANES, LANES), LANES)
            total[pl.ds(start, size), columns] += product(atile[slot, pl.ds(0, size), :], weights(columns))
            return carry

        lax.fori_loop(0, wide // LANES, lanes, 0)

    def own_jobs(count, size, job):
        def load(j, slot):
            term, which, start = job(j)
            block = owner(term)
            load_a(slot, size, block == z, place(block), start, which * half)
            load_b(slot, term, which)

        def step(j, carry):
            slot = lax.rem(j, 2)

            @pl.when(j + 1 < count)
            def _():
                load(j + 1, 1 - slot)

            wait_a(slot, size)
            wait_b(slot)
            multiply(acc, pl.multiple_of(job(j)[2], 8), size, slot, lambda columns: btile[slot, :, columns])
            return carry

        load(0, 0)
        lax.fori_loop(0, count, step, 0)

    def extra_jobs(i):
        size, start, buffer = sizes[i], starts[i], stage.at[i % 2]
        if i >= 2:
            remote(buffer.at[pl.ds(0, sizes[i - 2]), :], buffer.at[pl.ds(0, sizes[i - 2]), :], ("CX", i - 2), by_out).wait_send()
        buffer[pl.ds(0, size), :] = jnp.zeros((size, wide), jnp.float32)

        def load(j, slot):
            load_a(slot, size, jnp.bool_(False), 1 + j // 2, start, lax.rem(j, 2) * half)

        def step(j, carry):
            slot = lax.rem(j, 2)

            @pl.when(j + 1 < 4)
            def _():
                load(j + 1, 1 - slot)

            wait_a(slot, size)
            q = jnp.where(low, j // 2, 1 - j // 2)
            first = aligned(lax.rem(j, 2) * half)
            multiply(buffer, 0, size, slot, lambda columns: bx[q, pl.ds(first, half), columns])
            return carry

        load(0, 0)
        lax.fori_loop(0, 4, step, 0)
        copy = remote(buffer.at[pl.ds(0, size), :], cx.at[pl.ds(start, size), :], ("CX", i), by_out)
        copy.start()
        if i + 2 >= len(PARTS):
            sent.append(copy)

    def write(start, size, k):
        copy = pltpu.make_async_copy(acc.at[pl.ds(start, size), :], out.at[pl.ds(start, size), :], osem.at[k])
        copy.start()
        return copy

    chunks = range(len(PARTS))
    barrier = pltpu.get_barrier_semaphore()
    for device in (by_c, by_x, by_y, by_in):
        pl.semaphore_signal(barrier, inc=1, device_id=device, device_id_type=MESH)

    @pl.when(jnp.logical_not(edge))
    def _():
        pl.semaphore_signal(barrier, inc=1, device_id=by_out, device_id_type=MESH)

    pl.semaphore_wait(barrier, jnp.where(edge, 4, 5))

    def drain():
        for copy in sent:
            copy.wait_send()
        sent.clear()

    @pl.when(edge & near)
    def _():
        put(own_a(0), slot_a(0, 0), ("AE", 0), by_in)
        for p in range(PIECES):
            put(mine(p), main(1, layer, p), ("MX", p), by_x)
        for h in range(2):
            put(right.at[pl.ds(h * half, half), :], bmain.at[0, pl.ds(h * half, half), :], ("MC", h), by_c)
        for t in range(SUBS):
            got(extra_source(bmain.at[1], 1, t), ("XE", t))
            put(extra_source(bmain.at[1], 1, t), extra(core, 1, layer, t), ("X", t), by_in)
        for i in chunks[1:]:
            put(own_a(i), slot_a(0, i), ("AE", i), by_in)
        for h in range(2):
            got(bmain.at[0, pl.ds(h * half, half), :], ("MC", h))
        drain()

    @pl.when(edge & jnp.logical_not(near))
    def _():
        put(own_a(0), slot_a(0, 0), ("AE", 0), by_in)
        for t in range(SUBS):
            put(extra_source(right, 0, t), extra(core, 0, layer, t), ("X", t), by_in)
            put(extra_source(right, 1, t), extra_source(bmain.at[1], 1, t), ("XE", t), by_x)
        for i in chunks[1:]:
            put(own_a(i), slot_a(0, i), ("AE", i), by_in)
        for p in range(PIECES):
            got(main(1, layer, p), ("MX", p))
            put(main(1, layer, p), main(1, layer, p), ("MY", p), by_y)
            put(main(1, layer, p), main(2, layer, p), ("MF", p), by_c)
        for p in range(PIECES):
            got(main(1, flip, p), ("MY", p))
            put(main(1, flip, p), main(2, flip, p), ("MF", PIECES + p), by_c)
        for p in range(PIECES):
            got(main(2, layer, p), ("MF", p))
            got(main(2, flip, p), ("MF", PIECES + p))
        drain()

    @pl.when(edge)
    def _():
        acc[...] = jnp.zeros_like(acc)
        for i in chunks:
            got(slot_a(0, i), ("AB", i))
        size = max(sizes)
        count = rows // size
        own_jobs(4 * count, size, lambda j: (2 * farther + j // (2 * count), lax.rem(j // count, 2), lax.rem(j, count) * size))
        copies = []
        for i in chunks:
            view = cx.at[pl.ds(starts[i], sizes[i]), :]
            got(view, ("CX", i))
            acc[pl.ds(starts[i], sizes[i]), :] += view[...]
            copies.append(write(starts[i], sizes[i], i))
        for copy in copies:
            copy.wait()

    @pl.when(jnp.logical_not(edge))
    def _():
        def pieces_1(t):
            got(extra(core, spot, layer, t), ("X", t))
            put(extra(core, spot, layer, t), extra(core, spot, layer, t), ("P1", t), by_1)
            put(extra(core, spot, layer, t), extra(core, spot, layer, t), ("P2O", t), by_2)
            put(extra(core, spot, layer, t), extra(core, spot, layer, t), ("C0", t), by_c)

        def pieces_2(t):
            got(extra(core, *pair_1, t), ("P1", t))
            put(extra(core, *pair_1, t), extra(core, *pair_1, t), ("P2F", t), by_2)
            put(extra(core, *pair_1, t), extra(core, *pair_1, t), ("C1", t), by_c)

        def pieces_3(t):
            got(extra(core, *pair_2, t), ("P2O", t))
            put(extra(core, *pair_2, t), extra(core, *pair_2, t), ("C2", t), by_c)
            got(extra(core, *pair_3, t), ("P2F", t))
            put(extra(core, *pair_3, t), extra(core, *pair_3, t), ("C3", t), by_c)

        def ahead(i):
            got(slot_a(0, i), ("AE", i))
            put(slot_a(0, i), slot_a(2, i), ("AF", i), by_in)

        def across(i):
            put(own_a(i), slot_a(1, i), ("AO", i), by_in)

        def arrived(i):
            got(slot_a(1, i), ("AO", i))
            got(slot_a(2, i), ("AF", i))

        def take_x(p):
            got(main(1, layer, p), ("MX", p))
            put(main(1, layer, p), main(1, layer, p), ("MY", p), by_y)
            put(main(1, layer, p), main(2, layer, p), ("MF", p), by_c)

        def take_y(p):
            got(main(1, flip, p), ("MY", p))
            put(main(1, flip, p), main(2, flip, p), ("MF", PIECES + p), by_c)

        def near_units(i):
            own_jobs(4, sizes[i], lambda j: (j // 2, lax.rem(j, 2), starts[i]))

        for h in range(2):
            put(right.at[pl.ds(h * half, half), :], bmain.at[0, pl.ds(h * half, half), :], ("MC", h), by_c)
        across(0)
        across(1)
        for p in range(2):
            put(mine(p), main(1, layer, p), ("MX", p), by_x)
        for i in chunks:
            put(own_a(i), slot_a(0, i), ("AB", i), by_out)
        acc[...] = jnp.zeros_like(acc)
        take_x(0)
        ahead(0)
        across(2)
        across(3)
        pieces_1(0)
        pieces_2(0)
        pieces_1(1)
        for h in range(2):
            got(bmain.at[0, pl.ds(h * half, half), :], ("MC", h))
        pieces_3(0)
        arrived(0)
        near_units(0)
        pieces_2(1)
        take_x(1)
        for p in range(2, PIECES):
            put(mine(p), main(1, layer, p), ("MX", p), by_x)
        ahead(1)
        pieces_3(1)
        twin = 1 - core
        for t in range(SUBS):
            got(extra(twin, spot, layer, t), ("C0", t))
            got(extra(twin, *twin_1, t), ("C1", t))
            got(extra(twin, *twin_2, t), ("C2", t))
            got(extra(twin, *pair_3, t), ("C3", t))
        extra_jobs(0)
        ahead(2)
        take_y(0)
        take_y(1)
        arrived(1)
        extra_jobs(1)
        ahead(3)
        across(4)
        take_x(2)
        near_units(1)
        ahead(4)
        take_x(3)
        arrived(2)
        extra_jobs(2)
        near_units(2)
        for p in range(PIECES):
            got(main(2, layer, p), ("MF", p))
        big = sizes[0]
        own_jobs(6, big, lambda j: (2 + j // 3, layer, lax.rem(j, 3) * big))
        arrived(3)
        extra_jobs(3)
        for p in range(2, PIECES):
            take_y(p)
        for p in range(PIECES):
            got(main(2, flip, p), ("MF", PIECES + p))
        own_jobs(6, big, lambda j: (2 + j // 3, flip, lax.rem(j, 3) * big))
        own_jobs(8, sizes[3], lambda j: (j // 2, lax.rem(j, 2), starts[3]))
        early = write(0, starts[4], 0)
        arrived(4)
        extra_jobs(4)
        own_jobs(8, sizes[4], lambda j: (j // 2, lax.rem(j, 2), starts[4]))
        late = write(starts[4], sizes[4], 1)
        early.wait()
        late.wait()
        drain()


def line(left_factor, right_factor):
    depth, wide = right_factor.shape
    rows = left_factor.shape[0] // 2
    most = rows * max(PARTS) // sum(PARTS)
    half = depth // 2
    any_space = pl.BlockSpec(memory_space=pl.ANY)
    copies = len(KEYS)
    f32 = jnp.float32
    return pl.pallas_call(
        kernel,
        out_shape=(
            jax.ShapeDtypeStruct((rows, wide), f32),
            jax.ShapeDtypeStruct((3, rows, depth), f32),
            jax.ShapeDtypeStruct((3, depth, wide), f32),
        ),
        in_specs=[any_space] * 2,
        out_specs=[any_space] * 3,
        scratch_shapes=[
            pltpu.VMEM((2, depth, wide), f32),
            pltpu.VMEM((rows, wide), f32),
            pltpu.VMEM((rows, wide), f32),
            pltpu.VMEM((2, most, wide), f32),
            pltpu.VMEM((2, most, half), f32),
            pltpu.VMEM((2, half, wide), f32),
            pltpu.SemaphoreType.DMA((copies,)),
            pltpu.SemaphoreType.DMA((copies,)),
            pltpu.SemaphoreType.DMA((2,)),
            pltpu.SemaphoreType.DMA((2,)),
            pltpu.SemaphoreType.DMA((len(PARTS),)),
        ],
        compiler_params=pltpu.CompilerParams(collective_id=0, has_side_effects=True, vmem_limit_bytes=67043328),
        name="line",
    )(left_factor, right_factor)[0]


def solution(mesh):
    placed = (P("row", "col"), P("row", "col"))
    fits = (mesh.shape["row"], mesh.shape["col"], mesh.shape["layer"]) == (4, 4, 2)
    return jax.shard_map(
        line if fits else gathered,
        mesh=mesh,
        in_specs=placed,
        out_specs=P(("row", "layer"), "col"),
        check_vma=False,
    )
```

```python
import jax
import jax.numpy as jnp
from jax import lax
from jax.experimental import pallas as pl
from jax.experimental.pallas import tpu as pltpu
from jax.sharding import PartitionSpec as P

MESH = pl.DeviceIdType.MESH
EVEN = (1, 1, 1, 1)
PARTS = (4, 4, 4, 2, 2)
LANES = 512
PIECES = 8
SUBS = ((0, 2), (0, 3), (0, 0), (1, 0), (0, 1), (1, 1))


def product(left, right):
    return jnp.dot(
        left,
        right,
        precision=lax.Precision.HIGH,
        preferred_element_type=jnp.float32,
    )


def gathered(left_factor, right_factor):
    layers = lax.axis_size("layer")
    rows = left_factor.shape[0] // layers
    left = lax.dynamic_slice_in_dim(left_factor, lax.axis_index("layer") * rows, rows, 0)
    left = lax.all_gather(left, "col", axis=1, tiled=True)
    right = lax.all_gather(right_factor, "row", axis=0, tiled=True)
    return product(left, right)


def keys():
    n, table = 0, {}
    counts = dict(AE=len(PARTS), AB=len(EVEN), AO=len(EVEN), AF=len(PARTS), CX=len(PARTS))
    counts.update(X=len(SUBS), XE=len(SUBS), MC=2, MX=PIECES, MY=PIECES, MF=2 * PIECES)
    counts.update(PX=len(SUBS), PO=2, PF=2, C0=len(SUBS), C1=len(SUBS), C2=2, C3=2)
    for name, count in counts.items():
        for i in range(count):
            table[name, i] = n
            n += 1
    return table


KEYS = keys()


def kernel(left, right, out, abuf, bmain, bx, acc, exacc, atile, btile, ftile, send, recv, asem, bsem, osem):
    row, z, layer = (lax.axis_index(name) for name in ("row", "col", "layer"))
    rows, wide = acc.shape
    depth = right.shape[0]
    half = depth // 2
    tall = rows // len(EVEN)
    core = lax.rem(row, 2)
    low = z < 2
    edge = (z == 0) | (z == 3)
    near = (row // 2) == (z // 2)
    farther = jnp.where(near, 0, 1)
    row_x = lax.rem(row + 2, 4)
    row_c = row + 1 - 2 * core
    outer = jnp.where(low, z - 1, z + 1)
    inner = jnp.where(low, z + 1, z - 1)
    flip = 1 - layer
    by_x, by_c, by_y = {"row": row_x}, {"row": row_c}, {"layer": flip}
    by_out, by_in = {"col": outer}, {"col": inner}
    my_rows = layer * rows

    def remote(src, dst, key, device):
        k = KEYS[key]
        return pltpu.make_async_remote_copy(
            src_ref=src, dst_ref=dst, send_sem=send.at[k], recv_sem=recv.at[k], device_id=device, device_id_type=MESH
        )

    sent = []

    def put(src, dst, key, device):
        remote(src, dst, key, device).start()
        if (src.shape, key) not in sent:
            sent.append((src.shape, key))

    def got(dst, key):
        remote(dst, dst, key, by_c).wait_recv()

    def span(parts, i):
        size = rows // sum(parts)
        return sum(parts[:i]) * size, parts[i] * size

    def own_a(parts, i):
        start, size = span(parts, i)
        return left.at[pl.ds(my_rows + start, size), :]

    def slot_a(slot, parts, i):
        start, size = span(parts, i)
        return abuf.at[slot, pl.ds(start, size), :]

    def aligned(value):
        return pl.multiple_of(value, 128)

    cut = half // PIECES
    sub = half // 8

    def main(slot, which, p):
        return bmain.at[slot, pl.ds(aligned(which * half + p * cut), cut), :]

    def mine(p):
        return right.at[pl.ds(aligned(layer * half + p * cut), cut), :]

    def extra(q, far, which, t):
        return bx.at[q, pl.ds(aligned(which * half + far * (half // 2) + t * sub), sub), :]

    def extra_source(ref, far, k):
        other, t = SUBS[k]
        which = flip if other else layer
        return ref.at[pl.ds(aligned(which * half + far * (half // 2) + t * sub), sub), :]

    def extra_place(q, far, k):
        other, t = SUBS[k]
        return extra(q, far, flip if other else layer, t)

    spot = jnp.where(near, 1, 0)

    def load_a(view, sem, block, start, col):
        size, deep = view.shape
        where = pl.ds(aligned(col), deep)
        own = block == z
        turned = jnp.where(low, block, 3 - block)
        slot = jnp.maximum(turned - 1, 0)

        @pl.when(own)
        def _():
            pltpu.make_async_copy(left.at[pl.ds(my_rows + start, size), where], view, sem).start()

        @pl.when(jnp.logical_not(own))
        def _():
            pltpu.make_async_copy(abuf.at[slot, pl.ds(start, size), where], view, sem).start()

    def load_b(view, sem, term, first):
        where = pl.ds(aligned(first), view.shape[0])

        @pl.when(term == 0)
        def _():
            pltpu.make_async_copy(right.at[where, :], view, sem).start()

        @pl.when(term > 0)
        def _():
            pltpu.make_async_copy(bmain.at[jnp.maximum(term - 1, 0), where, :], view, sem).start()

    def landed(view, sem):
        pltpu.make_async_copy(view, view, sem).wait()

    def owner(term):
        return jnp.where(term == 0, row, jnp.where(term == 1, row_c, jnp.where(term == 2, row_x, 3 - row)))

    def multiply(total, start, lhs, weights):
        size = lhs.shape[0]

        def lanes(t, carry):
            columns = pl.ds(pl.multiple_of(t * LANES, LANES), LANES)
            total[pl.ds(start, size), columns] += product(lhs[...], weights(columns))
            return carry

        lax.fori_loop(0, wide // LANES, lanes, 0)

    def play(plan):
        runs, first = [], []
        for kind, *what in plan:
            if kind == "run":
                runs.append((what, [], []))
            elif not runs:
                first.append(what[0])
            else:
                runs[-1][1 if kind == "do" else 2].append(what[0])
        for act in first:
            act()
        base = 0
        for index, ((count, load, use), acts, after) in enumerate(runs):
            if index == 0:
                load(0, 0)
            following = runs[index + 1][0][1] if index + 1 < len(runs) else None

            def step(j, carry, count=count, load=load, use=use, acts=acts, following=following, base=base):
                slot = lax.rem(j + base, 2)

                @pl.when(j + 1 < count)
                def _():
                    load(j + 1, 1 - slot)

                @pl.when(j + 1 == count)
                def _():
                    for act in acts:
                        act()
                    if following is not None:
                        following(0, 1 - slot)

                use(j, slot)
                return carry

            lax.fori_loop(0, count, step, 0)
            for act in after:
                act()
            base = (base + count) % 2

    def own_jobs(count, job):
        def load(j, slot):
            term, first, start = job(j)
            load_a(atile.at[slot], asem.at[slot], owner(term), start, first)
            load_b(btile.at[slot], bsem.at[slot], term, first)

        def use(j, slot):
            landed(atile.at[slot], asem.at[slot])
            landed(btile.at[slot], bsem.at[slot])
            start = pl.multiple_of(job(j)[2], 8)
            multiply(acc, start, atile.at[slot], lambda columns: btile[slot, :, columns])

        return ("run", count, load, use)

    def far_jobs(count, job):
        deep = half // 2

        def load(j, slot):
            term, first, start = job(j)
            load_a(ftile.at[slot], asem.at[slot], owner(term), start, first)
            load_b(btile.at[slot, pl.ds(0, deep), :], bsem.at[slot], term, first)

        def use(j, slot):
            landed(ftile.at[slot], asem.at[slot])
            landed(btile.at[slot, pl.ds(0, deep), :], bsem.at[slot])
            start = pl.multiple_of(job(j)[2], 8)
            multiply(acc, start, ftile.at[slot], lambda columns: btile[slot, pl.ds(0, deep), columns])

        return ("run", count, load, use)

    def extra_jobs(count, size, job):
        def view(slot):
            return atile.at[slot, pl.ds(0, size), :]

        def load(j, slot):
            which, part, start = job(j)
            block = jnp.where(low, 2 + which, 1 - which)
            load_a(view(slot), asem.at[slot], block, start, part * half)

        def use(j, slot):
            which, part, start = job(j)
            landed(view(slot), asem.at[slot])
            q = jnp.where(low, which, 1 - which)
            first = aligned(part * half)
            multiply(exacc, pl.multiple_of(start, 8), view(slot), lambda columns: bx[q, pl.ds(first, half), columns])

        return ("run", count, load, use)

    def write(start, size, k):
        copy = pltpu.make_async_copy(acc.at[pl.ds(start, size), :], out.at[pl.ds(start, size), :], osem.at[k])
        copy.start()
        return copy

    chunks = range(len(PARTS))
    evens = range(len(EVEN))
    barrier = pltpu.get_barrier_semaphore()
    for device in (by_c, by_x, by_y, by_in):
        pl.semaphore_signal(barrier, inc=1, device_id=device, device_id_type=MESH)

    @pl.when(jnp.logical_not(edge))
    def _():
        pl.semaphore_signal(barrier, inc=1, device_id=by_out, device_id_type=MESH)

    pl.semaphore_wait(barrier, jnp.where(edge, 4, 5))

    def drain():
        for (high, broad), key in sent:
            view = (right if broad == wide else left).at[pl.ds(0, high), pl.ds(0, broad)]
            remote(view, view, key, by_c).wait_send()
        sent.clear()

    def edge_end():
        for i in evens:
            got(slot_a(0, EVEN, i), ("AB", i))
        count = len(EVEN)
        play([own_jobs(4 * count, lambda j: (2 * farther + j // (2 * count), lax.rem(j // count, 2) * half, lax.rem(j, count) * tall))])
        copies = []
        for i in chunks:
            start, size = span(PARTS, i)
            view = exacc.at[pl.ds(start, size), :]
            got(view, ("CX", i))
            acc[pl.ds(start, size), :] += view[...]
            copies.append(write(start, size, i))
        for copy in copies:
            copy.wait()
        drain()

    @pl.when(edge & near)
    def _():
        put(own_a(PARTS, 0), slot_a(0, PARTS, 0), ("AE", 0), by_in)
        for p in range(PIECES):
            put(mine(p), main(1, layer, p), ("MX", p), by_x)
        for h in range(2):
            put(right.at[pl.ds(h * half, half), :], bmain.at[0, pl.ds(h * half, half), :], ("MC", h), by_c)
        acc[...] = jnp.zeros_like(acc)
        for k in range(len(SUBS)):
            got(extra_source(bmain.at[1], 1, k), ("XE", k))
            put(extra_source(bmain.at[1], 1, k), extra_place(core, 1, k), ("X", k), by_in)
        for i in chunks[1:]:
            put(own_a(PARTS, i), slot_a(0, PARTS, i), ("AE", i), by_in)
        for h in range(2):
            got(bmain.at[0, pl.ds(h * half, half), :], ("MC", h))
        edge_end()

    @pl.when(edge & jnp.logical_not(near))
    def _():
        for k in range(len(SUBS)):
            if k == 4:
                put(own_a(PARTS, 0), slot_a(0, PARTS, 0), ("AE", 0), by_in)
            put(extra_source(right, 0, k), extra_place(core, 0, k), ("X", k), by_in)
            put(extra_source(right, 1, k), extra_source(bmain.at[1], 1, k), ("XE", k), by_x)
        for i in chunks[1:]:
            put(own_a(PARTS, i), slot_a(0, PARTS, i), ("AE", i), by_in)
        acc[...] = jnp.zeros_like(acc)
        for p in range(PIECES):
            got(main(1, layer, p), ("MX", p))
            put(main(1, layer, p), main(1, layer, p), ("MY", p), by_y)
            put(main(1, layer, p), main(2, layer, p), ("MF", p), by_c)
        for p in range(PIECES):
            got(main(1, flip, p), ("MY", p))
            put(main(1, flip, p), main(2, flip, p), ("MF", PIECES + p), by_c)
        for p in range(PIECES):
            got(main(2, layer, p), ("MF", p))
            got(main(2, flip, p), ("MF", PIECES + p))
        edge_end()

    @pl.when(jnp.logical_not(edge))
    def _():
        inner_term = jnp.where((row == 1) | (row == 2), 0, 1)
        outer_term = 1 - inner_term
        inner_far = 3 - inner_term
        outer_far = 2 + inner_term

        def from_outer(k):
            other, t = SUBS[k]
            view = extra_place(core, spot, k)
            got(view, ("X", k))
            put(view, view, ("PX", k), by_x)
            put(view, view, ("C0", k), by_c)
            if not other and t >= 2:
                put(view, view, ("PO", t - 2), by_y)

        def from_x(k):
            other, t = SUBS[k]
            view = extra_place(core, 1 - spot, k)
            got(view, ("PX", k))
            put(view, view, ("C1", k), by_c)
            if not other and t >= 2:
                put(view, view, ("PF", t - 2), by_y)

        def from_y(i):
            view = extra(core, spot, flip, i + 2)
            got(view, ("PO", i))
            put(view, view, ("C2", i), by_c)

        def across_y(i):
            view = extra(core, 1 - spot, flip, i + 2)
            got(view, ("PF", i))
            put(view, view, ("C3", i), by_c)

        def ahead(i):
            got(slot_a(0, PARTS, i), ("AE", i))
            put(slot_a(0, PARTS, i), slot_a(2, PARTS, i), ("AF", i), by_in)

        def take_x(p):
            got(main(1, layer, p), ("MX", p))
            put(main(1, layer, p), main(1, layer, p), ("MY", p), by_y)
            put(main(1, layer, p), main(2, layer, p), ("MF", p), by_c)

        def take_y(p):
            got(main(1, flip, p), ("MY", p))
            put(main(1, flip, p), main(2, flip, p), ("MF", PIECES + p), by_c)

        def inner_arrived(i):
            got(slot_a(1, EVEN, i), ("AO", i))

        def outer_arrived(i):
            got(slot_a(2, PARTS, i), ("AF", i))

        def inner_units(i):
            return own_jobs(2, lambda j: (inner_term, j * half, i * tall))

        def outer_units(i):
            return own_jobs(2, lambda j: (outer_term, j * half, i * tall))

        def far_units(terms, quarters, pairs):
            jobs = [(t, q, r) for t in terms for q in quarters for r in pairs]

            def pick(j, values):
                value = values[-1]
                for k in range(len(values) - 1):
                    value = jnp.where(j == k, values[k], value)
                return value

            firsts = [jnp.where(layer == (0 if q < 2 else 1), 0, 1) * half + (q % 2) * (half // 2) for q in range(4)]
            return far_jobs(
                len(jobs),
                lambda j: (
                    pick(j, [t for t, _, _ in jobs]),
                    pick(j, [firsts[q] for _, q, _ in jobs]),
                    pick(j, [r * 2 * tall for _, _, r in jobs]),
                ),
            )

        def send_sum(i):
            start, size = span(PARTS, i)
            put(exacc.at[pl.ds(start, size), :], exacc.at[pl.ds(start, size), :], ("CX", i), by_out)

        def outer_extra(i):
            start, size = span(PARTS, i)
            return extra_jobs(2, size, lambda j: (1, j, start))

        for h in range(2):
            put(right.at[pl.ds(h * half, half), :], bmain.at[0, pl.ds(h * half, half), :], ("MC", h), by_c)
        for i in evens:
            put(own_a(EVEN, i), slot_a(1, EVEN, i), ("AO", i), by_in)
        def give(p):
            put(mine(p), main(1, layer, p), ("MX", p), by_x)

        for p in range(2):
            give(p)
        for i in evens:
            put(own_a(EVEN, i), slot_a(0, EVEN, i), ("AB", i), by_out)
        exacc[...] = jnp.zeros_like(exacc)
        acc[...] = jnp.zeros_like(acc)

        def own_whole():
            for h in range(2):
                got(bmain.at[0, pl.ds(h * half, half), :], ("MC", h))

        def extras_whole():
            twin = 1 - core
            for k in range(len(SUBS)):
                got(extra_place(twin, spot, k), ("C0", k))
                got(extra_place(twin, 1 - spot, k), ("C1", k))
            for i in range(2):
                got(extra(twin, spot, flip, i + 2), ("C2", i))
                got(extra(twin, 1 - spot, flip, i + 2), ("C3", i))

        def whole(quarter):
            which, first = (layer, 0) if quarter < 2 else (flip, PIECES)
            for p in range(PIECES // 2 * (quarter % 2), PIECES // 2 * (quarter % 2 + 1)):
                got(main(2, which, p), ("MF", first + p))

        plan = []

        def do(act, *args):
            plan.append(("do", lambda: act(*args)))

        def then(act, *args):
            plan.append(("then", lambda: act(*args)))

        def only(side, acts):
            def act():
                @pl.when(near if side == "near" else jnp.logical_not(near))
                def _():
                    for what, *args in acts:
                        what(*args)

            plan.append(("do", act))

        only("far", [(from_outer, 0)])
        do(take_x, 0)
        do(take_x, 1)
        only("far", [(from_outer, 1)])
        only("near", [(give, 2)])
        do(own_whole)
        do(inner_arrived, 0)
        plan.append(inner_units(0))
        only("far", [(from_outer, 2), (from_outer, 3), (give, 2), (from_x, 0)])
        only("near", [(from_outer, 0), (from_x, 0), (from_outer, 1), (from_x, 1)])
        do(inner_arrived, 1)
        plan.append(inner_units(1))
        only("far", [(take_x, 2), (from_x, 1), (from_y, 0), (from_x, 2)])
        only("near", [(from_outer, 2), (from_x, 2), (from_y, 0), (from_outer, 3), (from_x, 3)])
        do(ahead, 0)
        do(inner_arrived, 2)
        plan.append(inner_units(2))
        do(from_y, 1)
        do(across_y, 0)
        do(from_outer, 4)
        only("far", [(from_x, 3)])
        only("near", [(take_x, 2)])
        do(across_y, 1)
        do(from_outer, 5)
        for p in range(3, PIECES):
            do(give, p)
        do(inner_arrived, 3)
        plan.append(inner_units(3))
        do(from_x, 4)
        do(from_x, 5)
        do(extras_whole)
        plan.append(extra_jobs(4, tall, lambda j: (0, lax.rem(j, 2), (j // 2) * tall)))
        do(ahead, 1)
        plan.append(extra_jobs(4, tall, lambda j: (0, lax.rem(j, 2), (2 + j // 2) * tall)))
        do(outer_arrived, 0)
        plan.append(outer_extra(0))
        then(send_sum, 0)
        do(take_x, 3)
        plan.append(outer_units(0))
        do(whole, 0)
        plan.append(far_units([inner_far], [0], [0, 1]))
        do(ahead, 2)
        do(take_x, 4)
        do(outer_arrived, 1)
        plan.append(outer_extra(1))
        then(send_sum, 1)
        plan.append(outer_units(1))
        for p in range(4):
            do(take_y, p)
        do(take_x, 5)
        do(whole, 2)
        plan.append(far_units([inner_far], [2], [0, 1]))
        plan.append(far_units([outer_far], [0, 2], [0]))
        do(take_x, 6)
        for i in chunks[3:]:
            do(ahead, i)
        do(outer_arrived, 2)
        plan.append(outer_extra(2))
        then(send_sum, 2)
        do(take_x, 7)
        plan.append(outer_units(2))
        do(whole, 1)
        plan.append(far_units([inner_far], [1], [0, 1]))
        do(outer_arrived, 3)
        plan.append(far_units([outer_far], [1], [0]))
        plan.append(outer_extra(3))
        then(send_sum, 3)
        plan.append(own_jobs(1, lambda j: (outer_far, layer * half, 2 * tall)))
        for p in range(4, PIECES):
            do(take_y, p)
        do(whole, 3)
        plan.append(far_units([inner_far], [3], [0, 1]))
        do(outer_arrived, 4)
        plan.append(far_units([outer_far], [3], [0]))
        then(write, 0, 2 * tall, 0)
        plan.append(outer_extra(4))
        then(send_sum, 4)
        plan.append(own_jobs(1, lambda j: (outer_far, flip * half, 2 * tall)))
        plan.append(outer_units(3))
        plan.append(own_jobs(2, lambda j: (outer_far, j * half, 3 * tall)))
        play(plan)
        write(2 * tall, 2 * tall, 1)
        for k in range(2):
            view = acc.at[pl.ds(0, 2 * tall), :]
            pltpu.make_async_copy(view, view, osem.at[k]).wait()
        drain()


def line(left_factor, right_factor):
    depth, wide = right_factor.shape
    rows = left_factor.shape[0] // 2
    tall = rows // len(EVEN)
    half = depth // 2
    any_space = pl.BlockSpec(memory_space=pl.ANY)
    copies = len(KEYS)
    f32 = jnp.float32
    return pl.pallas_call(
        kernel,
        out_shape=(
            jax.ShapeDtypeStruct((rows, wide), f32),
            jax.ShapeDtypeStruct((3, rows, depth), f32),
            jax.ShapeDtypeStruct((3, depth, wide), f32),
        ),
        in_specs=[any_space] * 2,
        out_specs=[any_space] * 3,
        scratch_shapes=[
            pltpu.VMEM((2, depth, wide), f32),
            pltpu.VMEM((rows, wide), f32),
            pltpu.VMEM((rows, wide), f32),
            pltpu.VMEM((2, tall, half), f32),
            pltpu.VMEM((2, half, wide), f32),
            pltpu.VMEM((2, 2 * tall, half // 2), f32),
            pltpu.SemaphoreType.DMA((copies,)),
            pltpu.SemaphoreType.DMA((copies,)),
            pltpu.SemaphoreType.DMA((2,)),
            pltpu.SemaphoreType.DMA((2,)),
            pltpu.SemaphoreType.DMA((len(PARTS),)),
        ],
        compiler_params=pltpu.CompilerParams(collective_id=0, has_side_effects=True, vmem_limit_bytes=67043328),
        name="line",
    )(left_factor, right_factor)[0]


def solution(mesh):
    placed = (P("row", "col"), P("row", "col"))
    fits = (mesh.shape["row"], mesh.shape["col"], mesh.shape["layer"]) == (4, 4, 2)
    return jax.shard_map(
        line if fits else gathered,
        mesh=mesh,
        in_specs=placed,
        out_specs=P(("row", "layer"), "col"),
        check_vma=False,
    )
```

```python
import jax
import jax.numpy as jnp
from jax import lax
from jax.experimental import pallas as pl
from jax.experimental.pallas import tpu as pltpu
from jax.sharding import PartitionSpec as P

MESH = pl.DeviceIdType.MESH
EVEN = (1, 1, 1, 1)
PARTS = (4, 4, 4, 2, 2)
OUTER = ((0, None), (1, None), (2, 0), (2, 1), (3, None), (4, 0), (4, 1))
LANES = 512
LAST = 3
PIECES = 8
SUBS = ((0, 2), (0, 3), (0, 0), (1, 0), (0, 1), (1, 1))


def product(left, right):
    return jnp.dot(
        left,
        right,
        precision=lax.Precision.HIGH,
        preferred_element_type=jnp.float32,
    )


def gathered(left_factor, right_factor):
    layers = lax.axis_size("layer")
    rows = left_factor.shape[0] // layers
    left = lax.dynamic_slice_in_dim(left_factor, lax.axis_index("layer") * rows, rows, 0)
    left = lax.all_gather(left, "col", axis=1, tiled=True)
    right = lax.all_gather(right_factor, "row", axis=0, tiled=True)
    return product(left, right)


def keys():
    n, table = 0, {}
    counts = dict(AE=len(OUTER), AB=len(EVEN), AO=len(EVEN), AF=len(OUTER), CX=len(PARTS) + LAST - 1)
    counts.update(X=len(SUBS), XE=len(SUBS), MC=2, MX=PIECES, MY=PIECES, MF=2 * PIECES)
    counts.update(PX=len(SUBS), PO=2, PF=2, C0=len(SUBS), C1=len(SUBS), C2=2, C3=2)
    for name, count in counts.items():
        for i in range(count):
            table[name, i] = n
            n += 1
    return table


KEYS = keys()


def sums(rows, wide):
    unit = rows // sum(PARTS)
    pieces = []
    for i, part in enumerate(PARTS):
        start = sum(PARTS[:i]) * unit
        if i < len(PARTS) - 1:
            pieces.append((("CX", i), start, part * unit, 0, wide))
        else:
            lanes = wide // LAST
            pieces += [(("CX", i + t), start, part * unit, t * lanes, lanes) for t in range(LAST)]
    return pieces


def kernel(left, right, acc, abuf, bmain, bx, exacc, atile, btile, ftile, send, recv, asem, bsem):
    row, z, layer = (lax.axis_index(name) for name in ("row", "col", "layer"))
    rows, wide = acc.shape
    depth = right.shape[0]
    half = depth // 2
    tall = rows // len(EVEN)
    core = lax.rem(row, 2)
    low = z < 2
    edge = (z == 0) | (z == 3)
    near = (row // 2) == (z // 2)
    farther = jnp.where(near, 0, 1)
    row_x = lax.rem(row + 2, 4)
    row_c = row + 1 - 2 * core
    outer = jnp.where(low, z - 1, z + 1)
    inner = jnp.where(low, z + 1, z - 1)
    flip = 1 - layer
    by_x, by_c, by_y = {"row": row_x}, {"row": row_c}, {"layer": flip}
    by_out, by_in = {"col": outer}, {"col": inner}
    my_rows = layer * rows

    def remote(src, dst, key, device):
        k = KEYS[key]
        return pltpu.make_async_remote_copy(
            src_ref=src, dst_ref=dst, send_sem=send.at[k], recv_sem=recv.at[k], device_id=device, device_id_type=MESH
        )

    sent = []

    def put(src, dst, key, device):
        remote(src, dst, key, device).start()
        if (src.shape, key) not in sent:
            sent.append((src.shape, key))

    def got(dst, key):
        remote(dst, dst, key, by_c).wait_recv()

    def span(parts, i):
        size = rows // sum(parts)
        return sum(parts[:i]) * size, parts[i] * size

    def own_a(parts, i):
        start, size = span(parts, i)
        return left.at[pl.ds(my_rows + start, size), :]

    def slot_a(slot, parts, i):
        start, size = span(parts, i)
        return abuf.at[slot, pl.ds(start, size), :]

    def side(part):
        return lax.rem(layer + part, 2)

    def piece(ref, offset, k):
        i, part = OUTER[k]
        start, size = span(PARTS, i)
        where = pl.ds(0, depth) if part is None else pl.ds(aligned(side(part) * half), half)
        return ref.at[pl.ds(offset + start, size), where]

    def aligned(value):
        return pl.multiple_of(value, 128)

    cut = half // PIECES
    sub = half // 8

    def main(slot, which, p):
        return bmain.at[slot, pl.ds(aligned(which * half + p * cut), cut), :]

    def mine(p):
        return right.at[pl.ds(aligned(layer * half + p * cut), cut), :]

    def extra(q, far, which, t):
        return bx.at[q, pl.ds(aligned(which * half + far * (half // 2) + t * sub), sub), :]

    def extra_source(ref, far, k):
        other, t = SUBS[k]
        which = flip if other else layer
        return ref.at[pl.ds(aligned(which * half + far * (half // 2) + t * sub), sub), :]

    def extra_place(q, far, k):
        other, t = SUBS[k]
        return extra(q, far, flip if other else layer, t)

    spot = jnp.where(near, 1, 0)

    def load_a(view, sem, block, start, col):
        size, deep = view.shape
        where = pl.ds(aligned(col), deep)
        own = block == z
        turned = jnp.where(low, block, 3 - block)
        slot = jnp.maximum(turned - 1, 0)

        @pl.when(own)
        def _():
            pltpu.make_async_copy(left.at[pl.ds(my_rows + start, size), where], view, sem).start()

        @pl.when(jnp.logical_not(own))
        def _():
            pltpu.make_async_copy(abuf.at[slot, pl.ds(start, size), where], view, sem).start()

    def load_b(view, sem, term, first):
        where = pl.ds(aligned(first), view.shape[0])

        @pl.when(term == 0)
        def _():
            pltpu.make_async_copy(right.at[where, :], view, sem).start()

        @pl.when(term > 0)
        def _():
            pltpu.make_async_copy(bmain.at[jnp.maximum(term - 1, 0), where, :], view, sem).start()

    def landed(view, sem):
        pltpu.make_async_copy(view, view, sem).wait()

    def owner(term):
        return jnp.where(term == 0, row, jnp.where(term == 1, row_c, jnp.where(term == 2, row_x, 3 - row)))

    def multiply(total, start, lhs, weights):
        size = lhs.shape[0]

        def lanes(t, carry):
            columns = pl.ds(pl.multiple_of(t * LANES, LANES), LANES)
            total[pl.ds(start, size), columns] += product(lhs[...], weights(columns))
            return carry

        lax.fori_loop(0, wide // LANES, lanes, 0)

    def play(plan):
        runs, first = [], []
        for kind, *what in plan:
            if kind == "run":
                runs.append((what, [], []))
            elif not runs:
                first.append(what[0])
            else:
                runs[-1][1 if kind == "do" else 2].append(what[0])
        for act in first:
            act()
        base = 0
        for index, ((count, load, use), acts, after) in enumerate(runs):
            if index == 0:
                load(0, 0)
            following = runs[index + 1][0][1] if index + 1 < len(runs) else None

            def step(j, carry, count=count, load=load, use=use, acts=acts, following=following, base=base):
                slot = lax.rem(j + base, 2)

                @pl.when(j + 1 < count)
                def _():
                    load(j + 1, 1 - slot)

                @pl.when(j + 1 == count)
                def _():
                    for act in acts:
                        act()
                    if following is not None:
                        following(0, 1 - slot)

                use(j, slot)
                return carry

            lax.fori_loop(0, count, step, 0)
            for act in after:
                act()
            base = (base + count) % 2

    def own_jobs(count, job):
        def load(j, slot):
            term, first, start = job(j)
            load_a(atile.at[slot], asem.at[slot], owner(term), start, first)
            load_b(btile.at[slot], bsem.at[slot], term, first)

        def use(j, slot):
            landed(atile.at[slot], asem.at[slot])
            landed(btile.at[slot], bsem.at[slot])
            start = pl.multiple_of(job(j)[2], 8)
            multiply(acc, start, atile.at[slot], lambda columns: btile[slot, :, columns])

        return ("run", count, load, use)

    def far_jobs(count, job):
        deep = half // 2

        def load(j, slot):
            term, first, start = job(j)
            load_a(ftile.at[slot], asem.at[slot], owner(term), start, first)
            load_b(btile.at[slot, pl.ds(0, deep), :], bsem.at[slot], term, first)

        def use(j, slot):
            landed(ftile.at[slot], asem.at[slot])
            landed(btile.at[slot, pl.ds(0, deep), :], bsem.at[slot])
            start = pl.multiple_of(job(j)[2], 8)
            multiply(acc, start, ftile.at[slot], lambda columns: btile[slot, pl.ds(0, deep), columns])

        return ("run", count, load, use)

    def extra_jobs(count, size, job, pieces=()):
        def view(slot):
            return atile.at[slot, pl.ds(0, size), :]

        def load(j, slot):
            which, part, start = job(j)
            block = jnp.where(low, 2 + which, 1 - which)
            load_a(view(slot), asem.at[slot], block, start, side(part) * half)

        def use(j, slot):
            which, part, start = job(j)
            landed(view(slot), asem.at[slot])
            q = jnp.where(low, which, 1 - which)
            first = aligned(side(part) * half)
            if not pieces:
                multiply(exacc, pl.multiple_of(start, 8), view(slot), lambda columns: bx[q, pl.ds(first, half), columns])
            for key, top, high, begin, broad in pieces:
                where = (pl.ds(top, high), pl.ds(begin, broad))
                exacc[where] += product(view(slot)[...], bx[q, pl.ds(first, half), pl.ds(begin, broad)])
                put(exacc.at[where], exacc.at[where], key, by_out)

        return ("run", count, load, use)

    chunks = range(len(PARTS))
    evens = range(len(EVEN))
    barrier = pltpu.get_barrier_semaphore()
    for device in (by_c, by_x, by_y, by_in):
        pl.semaphore_signal(barrier, inc=1, device_id=device, device_id_type=MESH)

    @pl.when(jnp.logical_not(edge))
    def _():
        pl.semaphore_signal(barrier, inc=1, device_id=by_out, device_id_type=MESH)

    pl.semaphore_wait(barrier, jnp.where(edge, 4, 5))

    def drain():
        for (high, broad), key in sent:
            view = (right if broad == wide else left).at[pl.ds(0, high), pl.ds(0, broad)]
            remote(view, view, key, by_c).wait_send()
        sent.clear()

    def edge_end():
        for i in evens:
            got(slot_a(0, EVEN, i), ("AB", i))
        count = len(EVEN)
        play([own_jobs(4 * count, lambda j: (2 * farther + j // (2 * count), lax.rem(j // count, 2) * half, lax.rem(j, count) * tall))])
        for key, start, size, first, broad in sums(rows, wide):
            where = (pl.ds(start, size), pl.ds(first, broad))
            got(exacc.at[where], key)
            acc[where] += exacc[where]
        drain()

    @pl.when(edge & near)
    def _():
        put(piece(left, my_rows, 0), piece(abuf.at[0], 0, 0), ("AE", 0), by_in)
        for p in range(PIECES):
            put(mine(p), main(1, layer, p), ("MX", p), by_x)
        for h in range(2):
            put(right.at[pl.ds(h * half, half), :], bmain.at[0, pl.ds(h * half, half), :], ("MC", h), by_c)
        acc[...] = jnp.zeros_like(acc)
        for k in range(len(SUBS)):
            got(extra_source(bmain.at[1], 1, k), ("XE", k))
            put(extra_source(bmain.at[1], 1, k), extra_place(core, 1, k), ("X", k), by_in)
        for k in range(1, len(OUTER)):
            put(piece(left, my_rows, k), piece(abuf.at[0], 0, k), ("AE", k), by_in)
        for h in range(2):
            got(bmain.at[0, pl.ds(h * half, half), :], ("MC", h))
        edge_end()

    @pl.when(edge & jnp.logical_not(near))
    def _():
        for k in range(len(SUBS)):
            if k == 4:
                put(piece(left, my_rows, 0), piece(abuf.at[0], 0, 0), ("AE", 0), by_in)
            put(extra_source(right, 0, k), extra_place(core, 0, k), ("X", k), by_in)
            put(extra_source(right, 1, k), extra_source(bmain.at[1], 1, k), ("XE", k), by_x)
        for k in range(1, len(OUTER)):
            put(piece(left, my_rows, k), piece(abuf.at[0], 0, k), ("AE", k), by_in)
        acc[...] = jnp.zeros_like(acc)
        for p in range(PIECES):
            got(main(1, layer, p), ("MX", p))
            put(main(1, layer, p), main(1, layer, p), ("MY", p), by_y)
            put(main(1, layer, p), main(2, layer, p), ("MF", p), by_c)
        for p in range(PIECES):
            got(main(1, flip, p), ("MY", p))
            put(main(1, flip, p), main(2, flip, p), ("MF", PIECES + p), by_c)
        for p in range(PIECES):
            got(main(2, layer, p), ("MF", p))
            got(main(2, flip, p), ("MF", PIECES + p))
        edge_end()

    @pl.when(jnp.logical_not(edge))
    def _():
        inner_term = jnp.where((row == 1) | (row == 2), 0, 1)
        outer_term = 1 - inner_term
        inner_far = 3 - inner_term
        outer_far = 2 + inner_term

        def from_outer(k):
            other, t = SUBS[k]
            view = extra_place(core, spot, k)
            got(view, ("X", k))
            put(view, view, ("PX", k), by_x)
            put(view, view, ("C0", k), by_c)
            if not other and t >= 2:
                put(view, view, ("PO", t - 2), by_y)

        def from_x(k):
            other, t = SUBS[k]
            view = extra_place(core, 1 - spot, k)
            got(view, ("PX", k))
            put(view, view, ("C1", k), by_c)
            if not other and t >= 2:
                put(view, view, ("PF", t - 2), by_y)

        def from_y(i):
            view = extra(core, spot, flip, i + 2)
            got(view, ("PO", i))
            put(view, view, ("C2", i), by_c)

        def across_y(i):
            view = extra(core, 1 - spot, flip, i + 2)
            got(view, ("PF", i))
            put(view, view, ("C3", i), by_c)

        def ahead(k):
            got(piece(abuf.at[0], 0, k), ("AE", k))
            put(piece(abuf.at[0], 0, k), piece(abuf.at[2], 0, k), ("AF", k), by_in)

        def take_x(p):
            got(main(1, layer, p), ("MX", p))
            put(main(1, layer, p), main(1, layer, p), ("MY", p), by_y)
            put(main(1, layer, p), main(2, layer, p), ("MF", p), by_c)

        def take_y(p):
            got(main(1, flip, p), ("MY", p))
            put(main(1, flip, p), main(2, flip, p), ("MF", PIECES + p), by_c)

        def inner_arrived(i):
            got(slot_a(1, EVEN, i), ("AO", i))

        def outer_arrived(k):
            got(piece(abuf.at[2], 0, k), ("AF", k))

        def inner_units(i):
            return own_jobs(2, lambda j: (inner_term, j * half, i * tall))

        def outer_units(i, parts=(0, 1)):
            return own_jobs(len(parts), lambda j: (outer_term, side(parts[0] + j) * half, i * tall))

        def pick(j, values):
            value = values[-1]
            for k in range(len(values) - 1):
                value = jnp.where(j == k, values[k], value)
            return value

        def far_units(terms, quarters, pairs):
            return far_list([(t, q, r) for t in terms for q in quarters for r in pairs])

        def far_list(jobs):
            firsts = [jnp.where(layer == (0 if q < 2 else 1), 0, 1) * half + (q % 2) * (half // 2) for q in range(4)]
            return far_jobs(
                len(jobs),
                lambda j: (
                    pick(j, [t for t, _, _ in jobs]),
                    pick(j, [firsts[q] for _, q, _ in jobs]),
                    pick(j, [r * 2 * tall for _, _, r in jobs]),
                ),
            )

        def send_sum(i):
            start, size = span(PARTS, i)
            put(exacc.at[pl.ds(start, size), :], exacc.at[pl.ds(start, size), :], ("CX", i), by_out)

        def outer_extra(i, parts=(0, 1)):
            start, size = span(PARTS, i)
            last = [piece for piece in sums(rows, wide) if piece[1] == start] if i == len(PARTS) - 1 and 1 in parts else ()
            return extra_jobs(len(parts), size, lambda j: (1, parts[0] + j, start), last)

        for h in range(2):
            put(right.at[pl.ds(h * half, half), :], bmain.at[0, pl.ds(h * half, half), :], ("MC", h), by_c)
        for i in evens:
            put(own_a(EVEN, i), slot_a(1, EVEN, i), ("AO", i), by_in)
        def give(p):
            put(mine(p), main(1, layer, p), ("MX", p), by_x)

        for p in range(2):
            give(p)
        for i in evens:
            put(own_a(EVEN, i), slot_a(0, EVEN, i), ("AB", i), by_out)
        exacc[...] = jnp.zeros_like(exacc)
        acc[...] = jnp.zeros_like(acc)

        def own_whole():
            for h in range(2):
                got(bmain.at[0, pl.ds(h * half, half), :], ("MC", h))

        def extras_whole():
            twin = 1 - core
            for k in range(len(SUBS)):
                got(extra_place(twin, spot, k), ("C0", k))
                got(extra_place(twin, 1 - spot, k), ("C1", k))
            for i in range(2):
                got(extra(twin, spot, flip, i + 2), ("C2", i))
                got(extra(twin, 1 - spot, flip, i + 2), ("C3", i))

        def whole(quarter):
            which, first = (layer, 0) if quarter < 2 else (flip, PIECES)
            for p in range(PIECES // 2 * (quarter % 2), PIECES // 2 * (quarter % 2 + 1)):
                got(main(2, which, p), ("MF", first + p))

        plan = []

        def do(act, *args):
            plan.append(("do", lambda: act(*args)))

        def then(act, *args):
            plan.append(("then", lambda: act(*args)))

        def only(side, acts):
            def act():
                @pl.when(near if side == "near" else jnp.logical_not(near))
                def _():
                    for what, *args in acts:
                        what(*args)

            plan.append(("do", act))

        only("far", [(from_outer, 0)])
        do(take_x, 0)
        do(take_x, 1)
        only("far", [(from_outer, 1)])
        only("near", [(give, 2)])
        do(own_whole)
        do(inner_arrived, 0)
        plan.append(inner_units(0))
        only("far", [(from_outer, 2), (from_outer, 3), (give, 2), (from_x, 0)])
        only("near", [(from_outer, 0), (from_x, 0), (from_outer, 1), (from_x, 1)])
        do(inner_arrived, 1)
        plan.append(inner_units(1))
        only("far", [(take_x, 2), (from_x, 1), (from_y, 0), (from_x, 2)])
        only("near", [(from_outer, 2), (from_x, 2), (from_y, 0), (from_outer, 3), (from_x, 3)])
        do(ahead, 0)
        do(inner_arrived, 2)
        plan.append(inner_units(2))
        do(from_y, 1)
        do(across_y, 0)
        do(from_outer, 4)
        only("far", [(from_x, 3)])
        only("near", [(take_x, 2)])
        do(across_y, 1)
        do(from_outer, 5)
        for p in range(3, PIECES):
            do(give, p)
        do(inner_arrived, 3)
        plan.append(inner_units(3))
        do(from_x, 4)
        do(from_x, 5)
        do(extras_whole)
        plan.append(extra_jobs(4, tall, lambda j: (0, lax.rem(j, 2), (j // 2) * tall)))
        do(ahead, 1)
        plan.append(extra_jobs(4, tall, lambda j: (0, lax.rem(j, 2), (2 + j // 2) * tall)))
        do(outer_arrived, 0)
        plan.append(outer_extra(0))
        then(send_sum, 0)
        do(take_x, 3)
        do(ahead, 2)
        plan.append(outer_units(0))
        do(whole, 0)
        plan.append(far_units([inner_far], [0], [0, 1]))
        do(take_x, 4)
        do(ahead, 3)
        do(outer_arrived, 1)
        plan.append(outer_extra(1))
        then(send_sum, 1)
        plan.append(outer_units(1))
        for p in range(4):
            do(take_y, p)
        do(take_x, 5)
        do(whole, 2)
        plan.append(far_units([inner_far], [2], [0, 1]))
        do(ahead, 4)
        plan.append(far_units([outer_far], [0, 2], [0]))
        do(take_x, 6)
        do(outer_arrived, 2)
        plan.append(outer_extra(2, (0,)))
        do(ahead, 5)
        plan.append(outer_units(2, (0,)))
        do(ahead, 6)
        do(outer_arrived, 3)
        plan.append(outer_extra(2, (1,)))
        then(send_sum, 2)
        plan.append(outer_units(2, (1,)))
        do(take_x, 7)
        do(take_y, 4)
        do(whole, 1)
        plan.append(far_units([inner_far], [1], [0, 1]))
        plan.append(far_units([outer_far], [1], [0]))
        plan.append(own_jobs(1, lambda j: (outer_far, layer * half, 2 * tall)))
        do(take_y, 5)
        do(outer_arrived, 4)
        plan.append(outer_extra(3))
        then(send_sum, 3)
        do(take_y, 6)
        do(outer_arrived, 5)
        plan.append(outer_extra(4, (0,)))
        plan.append(own_jobs(2, lambda j: (jnp.where(j == 0, outer_term, outer_far), layer * half, 3 * tall)))
        do(take_y, 7)
        do(outer_arrived, 6)
        plan.append(outer_extra(4, (1,)))
        do(whole, 3)
        plan.append(far_list([(inner_far, 3, 0), (inner_far, 3, 1), (outer_far, 3, 0), (outer_far, 2, 1), (outer_far, 3, 1)]))
        plan.append(outer_units(3, (1,)))
        play(plan)
        drain()


def line(left_factor, right_factor):
    depth, wide = right_factor.shape
    rows = left_factor.shape[0] // 2
    tall = rows // len(EVEN)
    half = depth // 2
    any_space = pl.BlockSpec(memory_space=pl.ANY)
    copies = len(KEYS)
    f32 = jnp.float32
    return pl.pallas_call(
        kernel,
        out_shape=(
            pltpu.VMEM((rows, wide), f32),
            jax.ShapeDtypeStruct((3, rows, depth), f32),
            jax.ShapeDtypeStruct((3, depth, wide), f32),
        ),
        in_specs=[any_space] * 2,
        out_specs=[pl.BlockSpec(memory_space=pltpu.VMEM), any_space, any_space],
        scratch_shapes=[
            pltpu.VMEM((2, depth, wide), f32),
            pltpu.VMEM((rows, wide), f32),
            pltpu.VMEM((2, tall, half), f32),
            pltpu.VMEM((2, half, wide), f32),
            pltpu.VMEM((2, 2 * tall, half // 2), f32),
            pltpu.SemaphoreType.DMA((copies,)),
            pltpu.SemaphoreType.DMA((copies,)),
            pltpu.SemaphoreType.DMA((2,)),
            pltpu.SemaphoreType.DMA((2,)),
        ],
        compiler_params=pltpu.CompilerParams(collective_id=0, has_side_effects=True, vmem_limit_bytes=56500000),
        name="line",
    )(left_factor, right_factor)[0]


def solution(mesh):
    placed = (P("row", "col"), P("row", "col"))
    fits = (mesh.shape["row"], mesh.shape["col"], mesh.shape["layer"]) == (4, 4, 2)
    return jax.shard_map(
        line if fits else gathered,
        mesh=mesh,
        in_specs=placed,
        out_specs=P(("row", "layer"), "col"),
        check_vma=False,
    )
```

```python
import jax
import jax.numpy as jnp
from jax import lax
from jax.experimental import pallas as pl
from jax.experimental.pallas import tpu as pltpu
from jax.sharding import PartitionSpec as P

MESH = pl.DeviceIdType.MESH
EVEN = (1, 1, 1, 1)
PARTS = (4, 4, 2, 2, 2, 2)
OUTER = ((0, None), (1, None), (2, None), (3, None), (4, None), (5, 0), (5, 1))
LANES = 512
LAST = 3
PIECES = 8
SUBS = ((0, 2), (0, 3), (0, 0), (1, 0), (0, 1), (1, 1))


def product(left, right):
    return jnp.dot(
        left,
        right,
        precision=lax.Precision.HIGH,
        preferred_element_type=jnp.float32,
    )


def gathered(left_factor, right_factor):
    layers = lax.axis_size("layer")
    rows = left_factor.shape[0] // layers
    left = lax.dynamic_slice_in_dim(left_factor, lax.axis_index("layer") * rows, rows, 0)
    left = lax.all_gather(left, "col", axis=1, tiled=True)
    right = lax.all_gather(right_factor, "row", axis=0, tiled=True)
    return product(left, right)


def keys():
    n, table = 0, {}
    counts = dict(AE=len(OUTER), AB=len(EVEN), AO=len(EVEN), AF=len(OUTER), CX=len(PARTS) + LAST - 1)
    counts.update(X=len(SUBS), XE=len(SUBS), MC=2, MX=PIECES, MY=PIECES, MF=2 * PIECES)
    counts.update(PX=len(SUBS), PO=2, PF=2, C0=len(SUBS), C1=len(SUBS), C2=2, C3=2)
    for name, count in counts.items():
        for i in range(count):
            table[name, i] = n
            n += 1
    return table


KEYS = keys()


def sums(rows, wide):
    unit = rows // sum(PARTS)
    pieces = []
    for i, part in enumerate(PARTS):
        start = sum(PARTS[:i]) * unit
        if i < len(PARTS) - 1:
            pieces.append((("CX", i), start, part * unit, 0, wide))
        else:
            lanes = wide // LAST
            pieces += [(("CX", i + t), start, part * unit, t * lanes, lanes) for t in range(LAST)]
    return pieces


def kernel(left, right, acc, abuf, bmain, bx, exacc, atile, btile, ftile, send, recv, asem, bsem):
    row, z, layer = (lax.axis_index(name) for name in ("row", "col", "layer"))
    rows, wide = acc.shape
    depth = right.shape[0]
    half = depth // 2
    tall = rows // len(EVEN)
    core = lax.rem(row, 2)
    low = z < 2
    edge = (z == 0) | (z == 3)
    near = (row // 2) == (z // 2)
    farther = jnp.where(near, 0, 1)
    row_x = lax.rem(row + 2, 4)
    row_c = row + 1 - 2 * core
    outer = jnp.where(low, z - 1, z + 1)
    inner = jnp.where(low, z + 1, z - 1)
    flip = 1 - layer
    by_x, by_c, by_y = {"row": row_x}, {"row": row_c}, {"layer": flip}
    by_out, by_in = {"col": outer}, {"col": inner}
    my_rows = layer * rows

    def remote(src, dst, key, device):
        k = KEYS[key]
        return pltpu.make_async_remote_copy(
            src_ref=src, dst_ref=dst, send_sem=send.at[k], recv_sem=recv.at[k], device_id=device, device_id_type=MESH
        )

    sent = []

    def put(src, dst, key, device):
        remote(src, dst, key, device).start()
        if (src.shape, key) not in sent:
            sent.append((src.shape, key))

    def got(dst, key):
        remote(dst, dst, key, by_c).wait_recv()

    def span(parts, i):
        size = rows // sum(parts)
        return sum(parts[:i]) * size, parts[i] * size

    def own_a(parts, i):
        start, size = span(parts, i)
        return left.at[pl.ds(my_rows + start, size), :]

    def slot_a(slot, parts, i):
        start, size = span(parts, i)
        return abuf.at[slot, pl.ds(start, size), :]

    def side(part):
        return lax.rem(layer + part, 2)

    def piece(ref, offset, k):
        i, part = OUTER[k]
        start, size = span(PARTS, i)
        where = pl.ds(0, depth) if part is None else pl.ds(aligned(side(part) * half), half)
        return ref.at[pl.ds(offset + start, size), where]

    def aligned(value):
        return pl.multiple_of(value, 128)

    cut = half // PIECES
    sub = half // 8

    def main(slot, which, p):
        return bmain.at[slot, pl.ds(aligned(which * half + p * cut), cut), :]

    def mine(p):
        return right.at[pl.ds(aligned(layer * half + p * cut), cut), :]

    def extra(q, far, which, t):
        return bx.at[q, pl.ds(aligned(which * half + far * (half // 2) + t * sub), sub), :]

    def extra_source(ref, far, k):
        other, t = SUBS[k]
        which = flip if other else layer
        return ref.at[pl.ds(aligned(which * half + far * (half // 2) + t * sub), sub), :]

    def extra_place(q, far, k):
        other, t = SUBS[k]
        return extra(q, far, flip if other else layer, t)

    spot = jnp.where(near, 1, 0)

    def load_a(view, sem, block, start, col):
        size, deep = view.shape
        where = pl.ds(aligned(col), deep)
        own = block == z
        turned = jnp.where(low, block, 3 - block)
        slot = jnp.maximum(turned - 1, 0)

        @pl.when(own)
        def _():
            pltpu.make_async_copy(left.at[pl.ds(my_rows + start, size), where], view, sem).start()

        @pl.when(jnp.logical_not(own))
        def _():
            pltpu.make_async_copy(abuf.at[slot, pl.ds(start, size), where], view, sem).start()

    def load_b(view, sem, term, first):
        where = pl.ds(aligned(first), view.shape[0])

        @pl.when(term == 0)
        def _():
            pltpu.make_async_copy(right.at[where, :], view, sem).start()

        @pl.when(term > 0)
        def _():
            pltpu.make_async_copy(bmain.at[jnp.maximum(term - 1, 0), where, :], view, sem).start()

    def landed(view, sem):
        pltpu.make_async_copy(view, view, sem).wait()

    def owner(term):
        return jnp.where(term == 0, row, jnp.where(term == 1, row_c, jnp.where(term == 2, row_x, 3 - row)))

    def multiply(total, start, lhs, weights):
        size = lhs.shape[0]

        def lanes(t, carry):
            columns = pl.ds(pl.multiple_of(t * LANES, LANES), LANES)
            total[pl.ds(start, size), columns] += product(lhs[...], weights(columns))
            return carry

        lax.fori_loop(0, wide // LANES, lanes, 0)

    def play(plan):
        runs, first = [], []
        for kind, *what in plan:
            if kind == "run":
                runs.append((what, [], [], []))
            elif not runs:
                first.append(what[0])
            else:
                runs[-1][("do", "then", "gap").index(kind) + 1].append(what[0])
        for act in first:
            act()
        base = 0
        for index, ((count, load, use), acts, after, gap) in enumerate(runs):
            if index == 0:
                load(0, 0)
            following = runs[index + 1][0][1] if index + 1 < len(runs) else None

            def step(j, carry, count=count, load=load, use=use, acts=acts, following=None if gap else following, base=base):
                slot = lax.rem(j + base, 2)

                @pl.when(j + 1 < count)
                def _():
                    load(j + 1, 1 - slot)

                @pl.when(j + 1 == count)
                def _():
                    for act in acts:
                        act()
                    if following is not None:
                        following(0, 1 - slot)

                use(j, slot)
                return carry

            lax.fori_loop(0, count, step, 0)
            base = (base + count) % 2
            for act in after + gap:
                act()
            if gap:
                following(0, base)

    def own_jobs(count, job):
        def load(j, slot):
            term, first, start = job(j)
            load_a(atile.at[slot], asem.at[slot], owner(term), start, first)
            load_b(btile.at[slot], bsem.at[slot], term, first)

        def use(j, slot):
            landed(atile.at[slot], asem.at[slot])
            landed(btile.at[slot], bsem.at[slot])
            start = pl.multiple_of(job(j)[2], 8)
            multiply(acc, start, atile.at[slot], lambda columns: btile[slot, :, columns])

        return ("run", count, load, use)

    def far_jobs(count, job):
        deep = half // 2

        def load(j, slot):
            term, first, start = job(j)
            load_a(ftile.at[slot], asem.at[slot], owner(term), start, first)
            load_b(btile.at[slot, pl.ds(0, deep), :], bsem.at[slot], term, first)

        def use(j, slot):
            landed(ftile.at[slot], asem.at[slot])
            landed(btile.at[slot, pl.ds(0, deep), :], bsem.at[slot])
            start = pl.multiple_of(job(j)[2], 8)
            multiply(acc, start, ftile.at[slot], lambda columns: btile[slot, pl.ds(0, deep), columns])

        return ("run", count, load, use)

    def extra_jobs(count, size, job, pieces=()):
        def view(slot):
            return atile.at[slot, pl.ds(0, size), :]

        def load(j, slot):
            which, part, start = job(j)
            block = jnp.where(low, 2 + which, 1 - which)
            load_a(view(slot), asem.at[slot], block, start, side(part) * half)

        def use(j, slot):
            which, part, start = job(j)
            landed(view(slot), asem.at[slot])
            q = jnp.where(low, which, 1 - which)
            first = aligned(side(part) * half)
            if not pieces:
                multiply(exacc, pl.multiple_of(start, 8), view(slot), lambda columns: bx[q, pl.ds(first, half), columns])
            for key, top, high, begin, broad in pieces:
                where = (pl.ds(top, high), pl.ds(begin, broad))
                exacc[where] += product(view(slot)[...], bx[q, pl.ds(first, half), pl.ds(begin, broad)])
                put(exacc.at[where], exacc.at[where], key, by_out)

        return ("run", count, load, use)

    chunks = range(len(PARTS))
    evens = range(len(EVEN))
    barrier = pltpu.get_barrier_semaphore()
    for device in (by_c, by_x, by_y, by_in):
        pl.semaphore_signal(barrier, inc=1, device_id=device, device_id_type=MESH)

    @pl.when(jnp.logical_not(edge))
    def _():
        pl.semaphore_signal(barrier, inc=1, device_id=by_out, device_id_type=MESH)

    pl.semaphore_wait(barrier, jnp.where(edge, 4, 5))

    def drain():
        for (high, broad), key in sent:
            view = (right if broad == wide else left).at[pl.ds(0, high), pl.ds(0, broad)]
            remote(view, view, key, by_c).wait_send()
        sent.clear()

    def edge_end():
        for i in evens:
            got(slot_a(0, EVEN, i), ("AB", i))
        count = len(EVEN)
        play([own_jobs(4 * count, lambda j: (2 * farther + j // (2 * count), lax.rem(j // count, 2) * half, lax.rem(j, count) * tall))])
        for key, start, size, first, broad in sums(rows, wide):
            where = (pl.ds(start, size), pl.ds(first, broad))
            got(exacc.at[where], key)
            acc[where] += exacc[where]
        drain()

    @pl.when(edge & near)
    def _():
        put(piece(left, my_rows, 0), piece(abuf.at[0], 0, 0), ("AE", 0), by_in)
        for p in range(PIECES):
            put(mine(p), main(1, layer, p), ("MX", p), by_x)
        for h in range(2):
            put(right.at[pl.ds(h * half, half), :], bmain.at[0, pl.ds(h * half, half), :], ("MC", h), by_c)
        acc[...] = jnp.zeros_like(acc)
        for k in range(len(SUBS)):
            got(extra_source(bmain.at[1], 1, k), ("XE", k))
            put(extra_source(bmain.at[1], 1, k), extra_place(core, 1, k), ("X", k), by_in)
        for k in range(1, len(OUTER)):
            put(piece(left, my_rows, k), piece(abuf.at[0], 0, k), ("AE", k), by_in)
        for h in range(2):
            got(bmain.at[0, pl.ds(h * half, half), :], ("MC", h))
        edge_end()

    @pl.when(edge & jnp.logical_not(near))
    def _():
        for k in range(len(SUBS)):
            if k == 4:
                put(piece(left, my_rows, 0), piece(abuf.at[0], 0, 0), ("AE", 0), by_in)
            put(extra_source(right, 0, k), extra_place(core, 0, k), ("X", k), by_in)
            put(extra_source(right, 1, k), extra_source(bmain.at[1], 1, k), ("XE", k), by_x)
        for k in range(1, len(OUTER)):
            put(piece(left, my_rows, k), piece(abuf.at[0], 0, k), ("AE", k), by_in)
        acc[...] = jnp.zeros_like(acc)
        for p in range(PIECES):
            got(main(1, layer, p), ("MX", p))
            put(main(1, layer, p), main(1, layer, p), ("MY", p), by_y)
            put(main(1, layer, p), main(2, layer, p), ("MF", p), by_c)
        for p in range(PIECES):
            got(main(1, flip, p), ("MY", p))
            put(main(1, flip, p), main(2, flip, p), ("MF", PIECES + p), by_c)
        for p in range(PIECES):
            got(main(2, layer, p), ("MF", p))
            got(main(2, flip, p), ("MF", PIECES + p))
        edge_end()

    @pl.when(jnp.logical_not(edge))
    def _():
        inner_term = jnp.where((row == 1) | (row == 2), 0, 1)
        outer_term = 1 - inner_term
        inner_far = 3 - inner_term
        outer_far = 2 + inner_term

        def from_outer(k):
            other, t = SUBS[k]
            view = extra_place(core, spot, k)
            got(view, ("X", k))
            put(view, view, ("PX", k), by_x)
            put(view, view, ("C0", k), by_c)
            if not other and t >= 2:
                put(view, view, ("PO", t - 2), by_y)

        def from_x(k):
            other, t = SUBS[k]
            view = extra_place(core, 1 - spot, k)
            got(view, ("PX", k))
            put(view, view, ("C1", k), by_c)
            if not other and t >= 2:
                put(view, view, ("PF", t - 2), by_y)

        def from_y(i):
            view = extra(core, spot, flip, i + 2)
            got(view, ("PO", i))
            put(view, view, ("C2", i), by_c)

        def across_y(i):
            view = extra(core, 1 - spot, flip, i + 2)
            got(view, ("PF", i))
            put(view, view, ("C3", i), by_c)

        def ahead(k):
            got(piece(abuf.at[0], 0, k), ("AE", k))
            put(piece(abuf.at[0], 0, k), piece(abuf.at[2], 0, k), ("AF", k), by_in)

        def take_x(p):
            got(main(1, layer, p), ("MX", p))
            put(main(1, layer, p), main(1, layer, p), ("MY", p), by_y)
            put(main(1, layer, p), main(2, layer, p), ("MF", p), by_c)

        def take_y(p):
            got(main(1, flip, p), ("MY", p))
            put(main(1, flip, p), main(2, flip, p), ("MF", PIECES + p), by_c)

        def inner_arrived(i):
            got(slot_a(1, EVEN, i), ("AO", i))

        def outer_arrived(k):
            got(piece(abuf.at[2], 0, k), ("AF", k))

        def inner_units(i):
            return own_jobs(2, lambda j: (inner_term, j * half, i * tall))

        def outer_units(i, parts=(0, 1)):
            return own_jobs(len(parts), lambda j: (outer_term, side(parts[0] + j) * half, i * tall))

        def pick(j, values):
            value = values[-1]
            for k in range(len(values) - 1):
                value = jnp.where(j == k, values[k], value)
            return value

        def far_units(terms, quarters, pairs):
            return far_list([(t, q, r) for t in terms for q in quarters for r in pairs])

        def far_list(jobs):
            firsts = [jnp.where(layer == (0 if q < 2 else 1), 0, 1) * half + (q % 2) * (half // 2) for q in range(4)]
            return far_jobs(
                len(jobs),
                lambda j: (
                    pick(j, [t for t, _, _ in jobs]),
                    pick(j, [firsts[q] for _, q, _ in jobs]),
                    pick(j, [r * 2 * tall for _, _, r in jobs]),
                ),
            )

        def send_sum(i):
            start, size = span(PARTS, i)
            put(exacc.at[pl.ds(start, size), :], exacc.at[pl.ds(start, size), :], ("CX", i), by_out)

        def outer_extra(i, parts=(0, 1)):
            start, size = span(PARTS, i)
            last = [piece for piece in sums(rows, wide) if piece[1] == start] if i == len(PARTS) - 1 and 1 in parts else ()
            return extra_jobs(len(parts), size, lambda j: (1, parts[0] + j, start), last)

        for h in range(2):
            put(right.at[pl.ds(h * half, half), :], bmain.at[0, pl.ds(h * half, half), :], ("MC", h), by_c)
        for i in evens:
            put(own_a(EVEN, i), slot_a(1, EVEN, i), ("AO", i), by_in)
        def give(p):
            put(mine(p), main(1, layer, p), ("MX", p), by_x)

        for p in range(2):
            give(p)
        for i in evens:
            put(own_a(EVEN, i), slot_a(0, EVEN, i), ("AB", i), by_out)
        exacc[...] = jnp.zeros_like(exacc)
        acc[...] = jnp.zeros_like(acc)

        def own_whole():
            for h in range(2):
                got(bmain.at[0, pl.ds(h * half, half), :], ("MC", h))

        def extras_whole():
            twin = 1 - core
            for k in range(len(SUBS)):
                got(extra_place(twin, spot, k), ("C0", k))
                got(extra_place(twin, 1 - spot, k), ("C1", k))
            for i in range(2):
                got(extra(twin, spot, flip, i + 2), ("C2", i))
                got(extra(twin, 1 - spot, flip, i + 2), ("C3", i))

        def whole(quarter):
            which, first = (layer, 0) if quarter < 2 else (flip, PIECES)
            for p in range(PIECES // 2 * (quarter % 2), PIECES // 2 * (quarter % 2 + 1)):
                got(main(2, which, p), ("MF", first + p))

        plan = []

        def do(act, *args):
            plan.append(("do", lambda: act(*args)))

        def then(act, *args):
            plan.append(("then", lambda: act(*args)))

        def gap(act, *args):
            plan.append(("gap", lambda: act(*args)))

        def only(side, acts):
            def act():
                @pl.when(near if side == "near" else jnp.logical_not(near))
                def _():
                    for what, *args in acts:
                        what(*args)

            plan.append(("do", act))

        only("far", [(from_outer, 0)])
        do(take_x, 0)
        do(take_x, 1)
        only("far", [(from_outer, 1)])
        only("near", [(give, 2)])
        do(own_whole)
        do(inner_arrived, 0)
        plan.append(inner_units(0))
        only("far", [(from_outer, 2), (from_outer, 3), (give, 2), (from_x, 0)])
        only("near", [(from_outer, 0), (from_x, 0), (from_outer, 1), (from_x, 1)])
        do(inner_arrived, 1)
        plan.append(inner_units(1))
        only("far", [(take_x, 2), (from_x, 1), (from_y, 0), (from_x, 2)])
        only("near", [(from_outer, 2), (from_x, 2), (from_y, 0), (from_outer, 3), (from_x, 3)])
        do(ahead, 0)
        do(inner_arrived, 2)
        plan.append(inner_units(2))
        do(from_y, 1)
        do(across_y, 0)
        do(from_outer, 4)
        only("far", [(from_x, 3)])
        only("near", [(take_x, 2)])
        do(across_y, 1)
        do(from_outer, 5)
        for p in range(3, PIECES):
            do(give, p)
        do(inner_arrived, 3)
        plan.append(inner_units(3))
        do(from_x, 4)
        do(from_x, 5)
        do(extras_whole)
        plan.append(extra_jobs(4, tall, lambda j: (0, lax.rem(j, 2), (j // 2) * tall)))
        do(ahead, 1)
        plan.append(extra_jobs(4, tall, lambda j: (0, lax.rem(j, 2), (2 + j // 2) * tall)))
        do(outer_arrived, 0)
        plan.append(outer_extra(0))
        then(send_sum, 0)
        do(take_x, 3)
        do(ahead, 2)
        plan.append(outer_units(0))
        do(whole, 0)
        plan.append(far_units([inner_far], [0], [0, 1]))
        do(take_x, 4)
        do(ahead, 3)
        do(outer_arrived, 1)
        plan.append(outer_extra(1))
        then(send_sum, 1)
        plan.append(outer_units(1))
        for p in range(4):
            do(take_y, p)
        do(take_x, 5)
        do(whole, 2)
        plan.append(far_units([inner_far], [2], [0, 1]))
        do(ahead, 4)
        plan.append(far_units([outer_far], [0, 2], [0]))
        do(take_x, 6)
        do(outer_arrived, 2)
        plan.append(outer_extra(2))
        then(send_sum, 2)
        for k in (5, 6):
            gap(ahead, k)
        gap(outer_arrived, 3)
        plan.append(outer_extra(3))
        then(send_sum, 3)
        do(take_x, 7)
        plan.append(outer_units(2))
        do(take_y, 4)
        do(whole, 1)
        plan.append(far_list([(inner_far, 1, 0), (inner_far, 1, 1), (outer_far, 1, 0)]))
        gap(take_y, 5)
        gap(outer_arrived, 4)
        plan.append(outer_extra(4))
        then(send_sum, 4)
        do(take_y, 6)
        plan.append(own_jobs(1, lambda j: (outer_far, layer * half, 2 * tall)))
        gap(outer_arrived, 5)
        plan.append(outer_extra(5, (0,)))
        plan.append(own_jobs(2, lambda j: (jnp.where(j == 0, outer_term, outer_far), layer * half, 3 * tall)))
        do(take_y, 7)
        do(outer_arrived, 6)
        plan.append(outer_extra(5, (1,)))
        do(whole, 3)
        plan.append(far_list([(inner_far, 3, 0), (inner_far, 3, 1), (outer_far, 3, 0), (outer_far, 2, 1), (outer_far, 3, 1)]))
        plan.append(outer_units(3, (1,)))
        play(plan)
        drain()


def line(left_factor, right_factor):
    depth, wide = right_factor.shape
    rows = left_factor.shape[0] // 2
    tall = rows // len(EVEN)
    half = depth // 2
    any_space = pl.BlockSpec(memory_space=pl.ANY)
    copies = len(KEYS)
    f32 = jnp.float32
    return pl.pallas_call(
        kernel,
        out_shape=(
            pltpu.VMEM((rows, wide), f32),
            jax.ShapeDtypeStruct((3, rows, depth), f32),
            jax.ShapeDtypeStruct((3, depth, wide), f32),
        ),
        in_specs=[any_space] * 2,
        out_specs=[pl.BlockSpec(memory_space=pltpu.VMEM), any_space, any_space],
        scratch_shapes=[
            pltpu.VMEM((2, depth, wide), f32),
            pltpu.VMEM((rows, wide), f32),
            pltpu.VMEM((2, tall, half), f32),
            pltpu.VMEM((2, half, wide), f32),
            pltpu.VMEM((2, 2 * tall, half // 2), f32),
            pltpu.SemaphoreType.DMA((copies,)),
            pltpu.SemaphoreType.DMA((copies,)),
            pltpu.SemaphoreType.DMA((2,)),
            pltpu.SemaphoreType.DMA((2,)),
        ],
        compiler_params=pltpu.CompilerParams(collective_id=0, has_side_effects=True, vmem_limit_bytes=56500000),
        name="line",
    )(left_factor, right_factor)[0]


def solution(mesh):
    placed = (P("row", "col"), P("row", "col"))
    fits = (mesh.shape["row"], mesh.shape["col"], mesh.shape["layer"]) == (4, 4, 2)
    return jax.shard_map(
        line if fits else gathered,
        mesh=mesh,
        in_specs=placed,
        out_specs=P(("row", "layer"), "col"),
        check_vma=False,
    )
```
